32 devices in a mesh: rep: 1 (over z), tp: 4 (over y), sp: 8 (over x, core).
Axes of the slice: x: 4, y: 4, z: 1, core: 2. Of those that a mesh axis runs over, the one named last changes fastest.
The devices are a block of a 4x4x8 slice.
Arguments:
- x_tokens: bfloat16 [6144, 4096], P(('rep', 'sp'))
- positions: int32 [6144], P(('rep', 'sp'))
- gains: float32 [2, 4, 4096], replicated
- w_q: bfloat16 [2, 4096, 32, 128], P(None, None, 'tp')
- w_k: bfloat16 [2, 4096, 8, 128], P(None, None, 'tp')
- w_v: bfloat16 [2, 4096, 8, 128], P(None, None, 'tp')
- w_o: bfloat16 [2, 32, 128, 4096], P(None, 'tp')
- w_gate: bfloat16 [2, 4096, 14336], P(None, None, 'tp')
- w_up: bfloat16 [2, 4096, 14336], P(None, None, 'tp')
- w_down: bfloat16 [2, 14336, 4096], P(None, 'tp')
Outputs:
- output 1: bfloat16 [6144, 4096], P(('rep', 'sp'))
- output 2: bfloat16 [512, 32, 128], P('rep', ('tp', 'sp'))
- output 3: bfloat16 [512, 32, 128], P('rep', ('tp', 'sp'))
- output 4: bfloat16 [6144, 32, 128], P('rep', ('tp', 'sp'))
- output 5: bfloat16 [6144, 32, 128], P('rep', ('tp', 'sp'))
All inputs are finite; a program needn't handle non-finite values.
Results may differ from the reference program's by a relative error of at most 0.0162776.
Values are sent between devices in bfloat16 or wider.
A program may use at most 768 MiB of HBM per device.

```python
import jax
import jax.numpy as jnp
from jax import lax

D = 4096
HEADS = 32
KV_HEADS = 8
HEAD = 128
FF = 14336
TOKENS = 6144
WINDOW = 512
CACHE_HEADS = 32
REF_BLOCK = 64

GROUP_SIZE = HEADS // KV_HEADS
REPEAT = CACHE_HEADS // KV_HEADS
NORM_EPS = 1e-6
LOCAL_BASE = 10000.0
GLOBAL_BASE = 1000000.0


def setup_inputs(seed: int = 0, part: int = 0) -> dict:
    part_key = jax.random.fold_in(jax.random.key(seed), part)
    key_x, key_pos = jax.random.split(part_key, 2)
    weight_keys = jax.random.split(jax.random.key(seed + 1), 8)
    x_tokens = jax.random.normal(key_x, (TOKENS, D), jnp.float32).astype(jnp.bfloat16)
    start = jax.random.randint(key_pos, (), 0, 4096)
    positions = (start + jnp.arange(TOKENS)).astype(jnp.int32)
    gains = 1.0 + 0.25 * jax.random.normal(weight_keys[0], (2, 4, D), jnp.float32)

    def weight(key, shape, fan_in):
        return (jax.random.normal(key, shape, jnp.float32) * fan_in ** -0.5).astype(jnp.bfloat16)

    return {
        'x_tokens': x_tokens,
        'positions': positions,
        'gains': gains,
        'w_q': weight(weight_keys[1], (2, D, HEADS, HEAD), D),
        'w_k': weight(weight_keys[2], (2, D, KV_HEADS, HEAD), D),
        'w_v': weight(weight_keys[3], (2, D, KV_HEADS, HEAD), D),
        'w_o': weight(weight_keys[4], (2, HEADS, HEAD, D), HEADS * HEAD),
        'w_gate': weight(weight_keys[5], (2, D, FF), D),
        'w_up': weight(weight_keys[6], (2, D, FF), D),
        'w_down': weight(weight_keys[7], (2, FF, D), FF),
    }


def rms_norm(values, gain):
    wide = values.astype(jnp.float32)
    inv_rms = lax.rsqrt(jnp.mean(wide * wide, axis=-1, keepdims=True) + NORM_EPS)
    return wide * inv_rms * gain


def rotary(projected, positions, base):
    half = projected.shape[-1] // 2
    inv_freq = base ** (-jnp.arange(half, dtype=jnp.float32) / half)
    angles = positions.astype(jnp.float32)[..., None] * inv_freq
    cos_part = jnp.cos(angles)[..., None, :]
    sin_part = jnp.sin(angles)[..., None, :]
    first = projected[..., :half]
    second = projected[..., half:]
    return jnp.concatenate([first * cos_part - second * sin_part, second * cos_part + first * sin_part], axis=-1)


def attention(q_rot, k_rot, v_new, local):
    q_wide = q_rot.reshape(TOKENS, KV_HEADS, GROUP_SIZE, HEAD).astype(jnp.float32)
    k_wide = k_rot.astype(jnp.float32)
    v_wide = v_new.astype(jnp.float32)
    span = WINDOW + REF_BLOCK if local else TOKENS

    def one_block(block_id):
        q_start = block_id * REF_BLOCK
        q_tile = lax.dynamic_slice_in_dim(q_wide, q_start, REF_BLOCK, 0)
        q_idx = q_start + jnp.arange(REF_BLOCK)
        k_start = jnp.clip(q_start - WINDOW, 0, TOKENS - span) if local else 0
        k_tile = lax.dynamic_slice_in_dim(k_wide, k_start, span, 0)
        v_tile = lax.dynamic_slice_in_dim(v_wide, k_start, span, 0)
        k_idx = k_start + jnp.arange(span)
        allowed = k_idx[None, :] <= q_idx[:, None]
        if local:
            allowed = allowed & (q_idx[:, None] - k_idx[None, :] < WINDOW)
        scores = jnp.einsum('qhgd,khd->hgqk', q_tile, k_tile) * (HEAD ** -0.5)
        weights = jax.nn.softmax(jnp.where(allowed, scores, -1e30), axis=-1)
        weights = weights.astype(jnp.bfloat16).astype(jnp.float32)
        return jnp.einsum('hgqk,khd->qhgd', weights, v_tile).astype(jnp.bfloat16)

    blocks = lax.map(one_block, jnp.arange(TOKENS // REF_BLOCK))
    return blocks.reshape(TOKENS, HEADS * HEAD)


def layer(hidden, positions, gain, w_q, w_k, w_v, w_o, w_gate, w_up, w_down, local):
    base = LOCAL_BASE if local else GLOBAL_BASE
    u_norm = rms_norm(hidden, gain[0]).astype(jnp.bfloat16)
    q_proj = jnp.dot(u_norm, w_q.reshape(D, HEADS * HEAD), preferred_element_type=jnp.float32)
    k_proj = jnp.dot(u_norm, w_k.reshape(D, KV_HEADS * HEAD), preferred_element_type=jnp.float32)
    v_proj = jnp.dot(u_norm, w_v.reshape(D, KV_HEADS * HEAD), preferred_element_type=jnp.float32)
    q_rot = rotary(q_proj.reshape(TOKENS, HEADS, HEAD), positions, base).astype(jnp.bfloat16)
    k_rot = rotary(k_proj.reshape(TOKENS, KV_HEADS, HEAD), positions, base).astype(jnp.bfloat16)
    v_new = v_proj.reshape(TOKENS, KV_HEADS, HEAD).astype(jnp.bfloat16)
    attn_out = attention(q_rot, k_rot, v_new, local)
    o_sum = jnp.dot(attn_out, w_o.reshape(HEADS * HEAD, D), preferred_element_type=jnp.float32)
    x_mid = (hidden.astype(jnp.float32) + rms_norm(o_sum, gain[1])).astype(jnp.bfloat16)
    u_mlp = rms_norm(x_mid, gain[2]).astype(jnp.bfloat16)
    gate_pre = jnp.dot(u_mlp, w_gate, preferred_element_type=jnp.float32)
    up_pre = jnp.dot(u_mlp, w_up, preferred_element_type=jnp.float32)
    hidden_act = (jax.nn.silu(gate_pre) * up_pre).astype(jnp.bfloat16)
    m_sum = jnp.dot(hidden_act, w_down, preferred_element_type=jnp.float32)
    x_out = (x_mid.astype(jnp.float32) + rms_norm(m_sum, gain[3])).astype(jnp.bfloat16)
    k_cache = jnp.repeat(k_rot, REPEAT, axis=1)
    v_cache = jnp.repeat(v_new, REPEAT, axis=1)
    if local:
        return x_out, k_cache[TOKENS - WINDOW:], v_cache[TOKENS - WINDOW:]
    return x_out, k_cache, v_cache


def reference(x_tokens, positions, gains, w_q, w_k, w_v, w_o, w_gate, w_up, w_down):
    hidden, k_local, v_local = layer(x_tokens, positions, gains[0], w_q[0], w_k[0], w_v[0], w_o[0], w_gate[0], w_up[0], w_down[0], True)
    out_hidden, k_global, v_global = layer(hidden, positions, gains[1], w_q[1], w_k[1], w_v[1], w_o[1], w_gate[1], w_up[1], w_down[1], False)
    return out_hidden, k_local, v_local, k_global, v_global
```

```python
import functools
import math

import jax
import jax.numpy as jnp
from jax import lax
from jax.experimental import pallas as pl
from jax.experimental.pallas import tpu as pltpu
from jax.sharding import PartitionSpec as P

NORM_EPS = 1e-6
WINDOW = 512
Q_BLOCK = 256
LOCAL_BASE = 10000.0
GLOBAL_BASE = 1000000.0
CHUNKS = 2
PACK_ROWS = 512
NEG = -1e30
F32 = jnp.float32
BF16 = jnp.bfloat16


def rms_norm(values, gain):
    wide = values.astype(F32)
    inv_rms = lax.rsqrt(jnp.mean(wide * wide, axis=-1, keepdims=True) + NORM_EPS)
    return wide * inv_rms * gain


def rope_tables(positions, half, base):
    inv_freq = base ** (-jnp.arange(half, dtype=F32) / half)
    angles = positions.astype(F32)[:, None] * inv_freq
    cos_part, sin_part = jnp.cos(angles), jnp.sin(angles)
    return jnp.stack([jnp.concatenate([cos_part, cos_part], axis=1), jnp.concatenate([-sin_part, sin_part], axis=1)])


def pack_kernel(q_ref, k_ref, v_ref, out_ref):
    at = 0
    for ref in (q_ref, k_ref, v_ref):
        depth, heads, dim = ref.shape[1:]
        out_ref[:, at:at + heads * dim] = ref[0].reshape(depth, heads * dim)
        at += heads * dim


def pack_weights(w_q, w_k, w_v, layer):
    width, _, dim = w_q.shape[1:]
    heads = [w.shape[2] for w in (w_q, w_k, w_v)]
    depth = PACK_ROWS
    columns = sum(heads) * dim
    return pl.pallas_call(
        pack_kernel,
        grid=(width // depth,),
        in_specs=[pl.BlockSpec((1, depth, h, dim), lambda i: (layer, i, 0, 0)) for h in heads],
        out_specs=pl.BlockSpec((depth, columns), lambda i: (i, 0)),
        out_shape=jax.ShapeDtypeStruct((width, columns), BF16),
        compiler_params=pltpu.CompilerParams(vmem_limit_bytes=40 << 20),
        cost_estimate=pl.CostEstimate(flops=8 * width * columns, bytes_accessed=4 * width * columns, transcendentals=0),
        name='pack_weights',
    )(w_q, w_k, w_v)


def project_kernel(rotated, dim, u_ref, w_ref, table_ref, out_ref):
    product = jnp.dot(u_ref[...], w_ref[...], preferred_element_type=F32)
    heads = w_ref.shape[1] // dim

    @pl.when(pl.program_id(0) < rotated)
    def _():
        cos_part, sin_part = table_ref[0], table_ref[1]
        for h in range(heads):
            part = product[:, h * dim:(h + 1) * dim]
            out_ref[h] = (part * cos_part + pltpu.roll(part, dim // 2, 1) * sin_part).astype(BF16)

    @pl.when(pl.program_id(0) >= rotated)
    def _():
        for h in range(heads):
            out_ref[h] = product[:, h * dim:(h + 1) * dim].astype(BF16)


def project(u_norm, packed, tables, rotated_heads):
    rows, width = u_norm.shape
    dim = tables.shape[2]
    columns = packed.shape[1]
    step = 2
    return pl.pallas_call(
        functools.partial(project_kernel, rotated_heads // step, dim),
        grid=(columns // (step * dim),),
        in_specs=[pl.BlockSpec((rows, width), lambda i: (0, 0)), pl.BlockSpec((width, step * dim), lambda i: (0, i)),
                  pl.BlockSpec(tables.shape, lambda i: (0, 0, 0))],
        out_specs=pl.BlockSpec((step, rows, dim), lambda i: (i, 0, 0)),
        out_shape=jax.ShapeDtypeStruct((columns // dim, rows, dim), BF16),
        compiler_params=pltpu.CompilerParams(vmem_limit_bytes=40 << 20),
        cost_estimate=pl.CostEstimate(flops=2 * rows * width * columns, bytes_accessed=2 * width * (columns + rows), transcendentals=0),
        name='project',
    )(u_norm, packed, tables)


def local_kernel(scale2, first_ref, q_ref, k_ref, v_ref, out_ref):
    heads, rows, dim = q_ref.shape
    span = rows + WINDOW
    start = pl.multiple_of(pl.program_id(1) * rows, rows)
    k_tile = k_ref[0, pl.ds(start, span), :]
    v_tile = v_ref[0, pl.ds(start, span), :]
    q_idx = lax.broadcasted_iota(jnp.int32, (rows, span), 0)
    k_idx = lax.broadcasted_iota(jnp.int32, (rows, span), 1)
    allowed = (k_idx > q_idx) & (k_idx <= q_idx + WINDOW) & (k_idx + start >= first_ref[0])
    for head in range(heads):
        scores = lax.dot_general(q_ref[head], k_tile, (((1,), (1,)), ((), ())), preferred_element_type=F32) * scale2
        scores = jnp.where(allowed, scores, NEG)
        top = jnp.max(scores, axis=1, keepdims=True)
        weights = jnp.exp2(scores - top)
        weights = weights * (1.0 / jnp.sum(weights, axis=1, keepdims=True))
        out = jnp.dot(weights.astype(BF16), v_tile, preferred_element_type=F32)
        out_ref[:, head * dim:(head + 1) * dim] = out.astype(BF16)


def local_attention(first, qkv, kv_ext, kv_heads):
    tokens, dim = qkv.shape[1:]
    q_heads = qkv.shape[0] - 2 * kv_heads
    group = q_heads // kv_heads
    scale2 = dim ** -0.5 * math.log2(math.e)
    k_spec = pl.BlockSpec((1, WINDOW + tokens, dim), lambda h, i: (h, 0, 0))
    v_spec = pl.BlockSpec((1, WINDOW + tokens, dim), lambda h, i: (kv_heads + h, 0, 0))
    return pl.pallas_call(
        functools.partial(local_kernel, scale2),
        grid=(kv_heads, tokens // Q_BLOCK),
        in_specs=[pl.BlockSpec(memory_space=pltpu.SMEM), pl.BlockSpec((group, Q_BLOCK, dim), lambda h, i: (h, i, 0)),
                  k_spec, v_spec],
        out_specs=pl.BlockSpec((Q_BLOCK, group * dim), lambda h, i: (i, h)),
        out_shape=jax.ShapeDtypeStruct((tokens, q_heads * dim), BF16),
        compiler_params=pltpu.CompilerParams(vmem_limit_bytes=40 << 20),
        cost_estimate=pl.CostEstimate(flops=4 * tokens * q_heads * dim * (WINDOW + Q_BLOCK), bytes_accessed=8 * tokens * q_heads * dim,
                                      transcendentals=0),
        name='local_attention',
    )(first, qkv, kv_ext, kv_ext)


def global_kernel(scale2, chunk, k_block, q_ref, k_ref, v_ref, out_ref):
    rows, dim = q_ref.shape[2:]
    q_tile = q_ref[0, 0]

    def step(carry, k_tile, v_tile, mask):
        top, total, acc = carry
        scores = lax.dot_general(q_tile, k_tile, (((1,), (1,)), ((), ())), preferred_element_type=F32) * scale2
        if mask is not None:
            scores = jnp.where(mask, scores, NEG)
        new_top = jnp.maximum(top, jnp.max(scores, axis=1, keepdims=True))
        weights = jnp.exp2(scores - new_top)
        fix = jnp.exp2(top - new_top)
        total = total * fix + jnp.sum(weights, axis=1, keepdims=True)
        acc = acc * fix + jnp.dot(weights.astype(BF16), v_tile, preferred_element_type=F32)
        return new_top, total, acc

    shard = pl.program_id(0)
    base = pl.multiple_of(shard * k_block, k_block)
    width = (chunk + 1) * rows
    q_idx = lax.broadcasted_iota(jnp.int32, (rows, width), 0) + chunk * rows
    k_idx = lax.broadcasted_iota(jnp.int32, (rows, width), 1)
    carry = (jnp.full((rows, 1), NEG, F32), jnp.zeros((rows, 1), F32), jnp.zeros((rows, dim), F32))
    carry = step(carry, k_ref[pl.ds(base, width), :], v_ref[pl.ds(base, width), :], k_idx <= q_idx)

    def full(j, carry):
        at = pl.multiple_of(j * k_block, k_block)
        return step(carry, k_ref[pl.ds(at, k_block), :], v_ref[pl.ds(at, k_block), :], None)

    top, total, acc = lax.fori_loop(0, shard, full, carry)
    out_ref[0] = (acc / total).astype(BF16)


def global_attention(q_part, k_all, v_all, chunk):
    shards, _, rows, dim = q_part.shape
    total = k_all.shape[0]
    scale2 = dim ** -0.5 * math.log2(math.e)
    q_spec = pl.BlockSpec((1, 1, rows, dim), lambda s: (s, 0, 0, 0))
    out_spec = pl.BlockSpec((1, rows, dim), lambda s: (s, 0, 0))
    k_spec = pl.BlockSpec((total, dim), lambda s: (0, 0))
    return pl.pallas_call(
        functools.partial(global_kernel, scale2, chunk, total // shards),
        grid=(shards,),
        in_specs=[q_spec, k_spec, k_spec],
        out_specs=out_spec,
        out_shape=jax.ShapeDtypeStruct((shards, rows, dim), BF16),
        compiler_params=pltpu.CompilerParams(vmem_limit_bytes=40 << 20),
        cost_estimate=pl.CostEstimate(flops=4 * shards * rows * total * dim, bytes_accessed=8 * total * dim, transcendentals=0),
        name='global_attention',
    )(q_part, k_all, v_all)


def solution(mesh):
    sp_size = mesh.shape['sp']
    tp_size = mesh.shape['tp']

    barrier = lax.optimization_barrier

    def gather(rows):
        return lax.all_gather(rows, 'tp', axis=0, tiled=True)

    def finish(partial, residual, gain):
        summed = lax.psum_scatter(partial, 'tp', scatter_dimension=0, tiled=True)
        return (residual.astype(F32) + rms_norm(summed, gain)).astype(BF16)

    def mlp(u_mlp, w_gate, w_up, w_down):
        gate_pre = jnp.dot(u_mlp, w_gate, preferred_element_type=F32)
        up_pre = jnp.dot(u_mlp, w_up, preferred_element_type=F32)
        hidden_act = (jax.nn.silu(gate_pre) * up_pre).astype(BF16)
        return jnp.dot(hidden_act, w_down, preferred_element_type=F32)

    def after_attention(partial_of, residuals, gain, w_gate, w_up, w_down, send_of):
        mids, gathered, partials, sent = [], [], [], []
        for c in range(CHUNKS):
            o_partial = partial_of(c)
            if c > 0:
                gathered[-1], o_partial = barrier((gathered[-1], o_partial))
                partials.append(mlp(gathered[-1], w_gate, w_up, w_down))
            x_mid = finish(o_partial, residuals[c], gain[1])
            mids.append(x_mid)
            gathered.append(gather(rms_norm(x_mid, gain[2]).astype(BF16)))
        for c in range(CHUNKS):
            if c + 1 < CHUNKS:
                follow = gathered[-1]
                follow, partials[c] = barrier((follow, partials[c]))
                gathered[-1] = follow
            else:
                partials.append(mlp(gathered[-1], w_gate, w_up, w_down))
                sent[-1], partials[c] = barrier((sent[-1], partials[c]))
            done = finish(partials[c], mids[c], gain[3])
            mids[c] = done
            sent.append(gather(send_of(done)))
        return mids, sent

    def device_fn(x_loc, pos_loc, gains, w_q, w_k, w_v, w_o, w_gate, w_up, w_down):
        tp_idx = lax.axis_index('tp')
        sp_idx = lax.axis_index('sp')
        tokens, width = x_loc.shape
        rows = tokens // CHUNKS
        part = rows // tp_size
        heads_tp, dim = w_q.shape[2:]
        kv_tp = w_k.shape[2]
        repeat = sp_size // kv_tp
        w_o = barrier(w_o.reshape(w_o.shape[0], heads_tp * dim, width))

        tables = rope_tables(pos_loc, dim // 2, LOCAL_BASE)
        u_norm = rms_norm(x_loc, gains[0, 0]).astype(BF16)
        qkv = project(u_norm, pack_weights(w_q, w_k, w_v, 0), tables, heads_tp + kv_tp)
        kv = qkv[heads_tp:]
        tail = kv[:, tokens - WINDOW:]
        halo = lax.ppermute(tail, 'sp', [(i, i + 1) for i in range(sp_size - 1)])
        first = jnp.where(sp_idx == 0, WINDOW, 0).astype(jnp.int32).reshape(1)
        attn = local_attention(first, qkv, jnp.concatenate([halo, kv], axis=1), kv_tp)
        residuals = [lax.dynamic_slice_in_dim(x_loc, c * rows + tp_idx * part, part, 0) for c in range(CHUNKS)]
        hidden, u_next = after_attention(
            lambda c: jnp.dot(attn[c * rows:(c + 1) * rows], w_o[0], preferred_element_type=F32),
            residuals, gains[0], w_gate[0], w_up[0], w_down[0], lambda done: rms_norm(done, gains[1, 0]).astype(BF16))

        pairs = tail.reshape(2, kv_tp, WINDOW, dim)
        held = pairs[:, kv_tp - 1]
        for h in range(kv_tp - 1):
            owner = (h + 1) * repeat - 1
            held = jnp.where(sp_idx == owner, lax.ppermute(pairs[:, h], 'sp', [(sp_size - 1, owner)]), held)
        reach = repeat
        while reach > 1:
            moves = [(end - 1, end - 1 - reach // 2) for end in range(reach, sp_size + 1, reach)]
            moved = lax.ppermute(held, 'sp', moves)
            takes = (sp_idx + 1) % reach == reach // 2
            held = jnp.where(takes, moved, held)
            reach //= 2
        k_local = held[0][:, None, :]
        v_local = held[1][:, None, :]

        tables = rope_tables(pos_loc, dim // 2, GLOBAL_BASE)
        packed = pack_weights(w_q, w_k, w_v, 1)
        got = []
        for c in range(CHUNKS):
            qkv = project(u_next[c], packed, tables[:, c * rows:(c + 1) * rows], heads_tp + kv_tp)
            outgoing = jnp.stack([qkv[:heads_tp], jnp.repeat(qkv[heads_tp:heads_tp + kv_tp], repeat, axis=0),
                                  jnp.repeat(qkv[heads_tp + kv_tp:], repeat, axis=0)], axis=1)
            got.append(lax.all_to_all(outgoing, 'sp', 0, 0, tiled=True))
        k_all = jnp.concatenate([g[:, 1] for g in got], axis=1).reshape(sp_size * tokens, dim)
        v_all = jnp.concatenate([g[:, 2] for g in got], axis=1).reshape(sp_size * tokens, dim)

        def global_partial(c):
            back = lax.all_to_all(global_attention(got[c], k_all, v_all, c), 'sp', 0, 0, tiled=True)
            back = back.transpose(1, 0, 2).reshape(rows, heads_tp * dim)
            return jnp.dot(back, w_o[1], preferred_element_type=F32)

        _, outs = after_attention(global_partial, hidden, gains[1], w_gate[1], w_up[1], w_down[1], lambda done: done)
        return jnp.concatenate(outs, axis=0), k_local, v_local, k_all[:, None, :], v_all[:, None, :]

    token_spec = P(('rep', 'sp'), None)
    cache_spec = P('rep', ('tp', 'sp'), None)
    in_specs = (token_spec, P(('rep', 'sp')), P(), P(None, None, 'tp', None), P(None, None, 'tp', None),
                P(None, None, 'tp', None), P(None, 'tp', None, None), P(None, None, 'tp'), P(None, None, 'tp'),
                P(None, 'tp', None))
    out_specs = (token_spec, cache_spec, cache_spec, cache_spec, cache_spec)
    return jax.shard_map(device_fn, mesh=mesh, in_specs=in_specs, out_specs=out_specs, check_vma=False)
```

```python
import functools
import math

import jax
import jax.numpy as jnp
from jax import lax
from jax.experimental import pallas as pl
from jax.experimental.pallas import tpu as pltpu
from jax.sharding import PartitionSpec as P


NORM_EPS = 1e-6
WINDOW = 512
LOCAL_BASE = 10000.0
GLOBAL_BASE = 1000000.0
CHUNKS = 2
PACK_ROWS = 512
NEG = -1e30
F32 = jnp.float32
BF16 = jnp.bfloat16


def rms_norm(values, gain):
    wide = values.astype(F32)
    inv_rms = lax.rsqrt(jnp.mean(wide * wide, axis=-1, keepdims=True) + NORM_EPS)
    return wide * inv_rms * gain


def rope_tables(positions, half, base):
    inv_freq = base ** (-jnp.arange(half, dtype=F32) / half)
    angles = positions.astype(F32)[:, None] * inv_freq
    cos_part, sin_part = jnp.cos(angles), jnp.sin(angles)
    return jnp.stack([jnp.concatenate([cos_part, cos_part], axis=1), jnp.concatenate([-sin_part, sin_part], axis=1)])


def pack_kernel(q_ref, k_ref, v_ref, out_ref):
    at = 0
    for ref in (q_ref, k_ref, v_ref):
        depth, heads, dim = ref.shape[1:]
        out_ref[:, at:at + heads * dim] = ref[0].reshape(depth, heads * dim)
        at += heads * dim


def pack_weights(w_q, w_k, w_v, layer):
    width, _, dim = w_q.shape[1:]
    heads = [w.shape[2] for w in (w_q, w_k, w_v)]
    depth = PACK_ROWS
    columns = sum(heads) * dim
    return pl.pallas_call(
        pack_kernel,
        grid=(width // depth,),
        in_specs=[pl.BlockSpec((1, depth, h, dim), lambda i: (layer, i, 0, 0)) for h in heads],
        out_specs=pl.BlockSpec((depth, columns), lambda i: (i, 0)),
        out_shape=jax.ShapeDtypeStruct((width, columns), BF16),
        compiler_params=pltpu.CompilerParams(vmem_limit_bytes=40 << 20),
        cost_estimate=pl.CostEstimate(flops=8 * width * columns, bytes_accessed=4 * width * columns, transcendentals=0),
        name='pack_weights',
    )(w_q, w_k, w_v)


def project_kernel(rotated, dim, u_ref, w_ref, table_ref, out_ref):
    product = jnp.dot(u_ref[...], w_ref[...], preferred_element_type=F32)
    heads = w_ref.shape[1] // dim

    @pl.when(pl.program_id(0) < rotated)
    def _():
        cos_part, sin_part = table_ref[0], table_ref[1]
        for h in range(heads):
            part = product[:, h * dim:(h + 1) * dim]
            out_ref[h] = (part * cos_part + pltpu.roll(part, dim // 2, 1) * sin_part).astype(BF16)

    @pl.when(pl.program_id(0) >= rotated)
    def _():
        for h in range(heads):
            out_ref[h] = product[:, h * dim:(h + 1) * dim].astype(BF16)


def project(u_norm, packed, tables, rotated_heads):
    rows, width = u_norm.shape
    dim = tables.shape[2]
    columns = packed.shape[1]
    step = 2
    return pl.pallas_call(
        functools.partial(project_kernel, rotated_heads // step, dim),
        grid=(columns // (step * dim),),
        in_specs=[pl.BlockSpec((rows, width), lambda i: (0, 0)), pl.BlockSpec((width, step * dim), lambda i: (0, i)),
                  pl.BlockSpec(tables.shape, lambda i: (0, 0, 0))],
        out_specs=pl.BlockSpec((step, rows, dim), lambda i: (i, 0, 0)),
        out_shape=jax.ShapeDtypeStruct((columns // dim, rows, dim), BF16),
        compiler_params=pltpu.CompilerParams(vmem_limit_bytes=40 << 20),
        cost_estimate=pl.CostEstimate(flops=2 * rows * width * columns, bytes_accessed=2 * width * (columns + rows), transcendentals=0),
        name='project',
    )(u_norm, packed, tables)


def local_kernel(scale2, chunk, first_ref, q_ref, k_ref, v_ref, out_ref):
    heads, rows, dim = q_ref.shape
    span = rows + WINDOW
    start = chunk * rows
    k_tile = k_ref[0, pl.ds(start, span), :]
    v_tile = v_ref[0, pl.ds(start, span), :]
    q_idx = lax.broadcasted_iota(jnp.int32, (rows, span), 0)
    k_idx = lax.broadcasted_iota(jnp.int32, (rows, span), 1)
    allowed = (k_idx > q_idx) & (k_idx <= q_idx + WINDOW) & (k_idx + start >= first_ref[0])
    for head in range(heads):
        scores = lax.dot_general(q_ref[head], k_tile, (((1,), (1,)), ((), ())), preferred_element_type=F32) * scale2
        scores = jnp.where(allowed, scores, NEG)
        top = jnp.max(scores, axis=1, keepdims=True)
        weights = jnp.exp2(scores - top)
        weights = weights * (1.0 / jnp.sum(weights, axis=1, keepdims=True))
        out = jnp.dot(weights.astype(BF16), v_tile, preferred_element_type=F32)
        out_ref[:, head * dim:(head + 1) * dim] = out.astype(BF16)


def local_attention(first, qkv, kv_ext, kv_heads, chunk):
    tokens, dim = qkv.shape[1:]
    rows = tokens // CHUNKS
    q_heads = qkv.shape[0] - 2 * kv_heads
    group = q_heads // kv_heads
    scale2 = dim ** -0.5 * math.log2(math.e)
    k_spec = pl.BlockSpec((1, WINDOW + tokens, dim), lambda h: (h, 0, 0))
    v_spec = pl.BlockSpec((1, WINDOW + tokens, dim), lambda h: (kv_heads + h, 0, 0))
    return pl.pallas_call(
        functools.partial(local_kernel, scale2, chunk),
        grid=(kv_heads,),
        in_specs=[pl.BlockSpec(memory_space=pltpu.SMEM), pl.BlockSpec((group, rows, dim), lambda h: (h, chunk, 0)),
                  k_spec, v_spec],
        out_specs=pl.BlockSpec((rows, group * dim), lambda h: (0, h)),
        out_shape=jax.ShapeDtypeStruct((rows, q_heads * dim), BF16),
        compiler_params=pltpu.CompilerParams(vmem_limit_bytes=40 << 20),
        cost_estimate=pl.CostEstimate(flops=4 * rows * q_heads * dim * (WINDOW + rows), bytes_accessed=8 * rows * q_heads * dim,
                                      transcendentals=0),
        name='local_attention',
    )(first, qkv, kv_ext, kv_ext)


def global_kernel(scale2, chunk, k_block, q_ref, k_ref, v_ref, out_ref):
    rows, dim = q_ref.shape[2:]
    q_tile = q_ref[0, 0]

    def step(carry, k_tile, v_tile, mask):
        top, total, acc = carry
        scores = lax.dot_general(q_tile, k_tile, (((1,), (1,)), ((), ())), preferred_element_type=F32) * scale2
        if mask is not None:
            scores = jnp.where(mask, scores, NEG)
        new_top = jnp.maximum(top, jnp.max(scores, axis=1, keepdims=True))
        weights = jnp.exp2(scores - new_top)
        fix = jnp.exp2(top - new_top)
        total = total * fix + jnp.sum(weights, axis=1, keepdims=True)
        acc = acc * fix + jnp.dot(weights.astype(BF16), v_tile, preferred_element_type=F32)
        return new_top, total, acc

    shard = pl.program_id(0)
    base = pl.multiple_of(shard * k_block, k_block)
    width = (chunk + 1) * rows
    q_idx = lax.broadcasted_iota(jnp.int32, (rows, width), 0) + chunk * rows
    k_idx = lax.broadcasted_iota(jnp.int32, (rows, width), 1)
    carry = (jnp.full((rows, 1), NEG, F32), jnp.zeros((rows, 1), F32), jnp.zeros((rows, dim), F32))
    carry = step(carry, k_ref[pl.ds(base, width), :], v_ref[pl.ds(base, width), :], k_idx <= q_idx)

    def full(j, carry):
        at = pl.multiple_of(j * k_block, k_block)
        return step(carry, k_ref[pl.ds(at, k_block), :], v_ref[pl.ds(at, k_block), :], None)

    _, total, acc = lax.fori_loop(0, shard, full, carry)
    out_ref[0] = (acc / total).astype(BF16)


def global_attention(q_part, k_all, v_all, chunk):
    shards, _, rows, dim = q_part.shape
    total = k_all.shape[0]
    scale2 = dim ** -0.5 * math.log2(math.e)
    q_spec = pl.BlockSpec((1, 1, rows, dim), lambda s: (s, 0, 0, 0))
    out_spec = pl.BlockSpec((1, rows, dim), lambda s: (s, 0, 0))
    k_spec = pl.BlockSpec((total, dim), lambda s: (0, 0))
    return pl.pallas_call(
        functools.partial(global_kernel, scale2, chunk, total // shards),
        grid=(shards,),
        in_specs=[q_spec, k_spec, k_spec],
        out_specs=out_spec,
        out_shape=jax.ShapeDtypeStruct((shards, rows, dim), BF16),
        compiler_params=pltpu.CompilerParams(vmem_limit_bytes=40 << 20),
        cost_estimate=pl.CostEstimate(flops=4 * shards * rows * total * dim, bytes_accessed=8 * total * dim, transcendentals=0),
        name='global_attention',
    )(q_part, k_all, v_all)


def solution(mesh):
    sp_size = mesh.shape['sp']
    tp_size = mesh.shape['tp']

    barrier = lax.optimization_barrier

    def gather(rows):
        return lax.all_gather(rows, 'tp', axis=0, tiled=True)

    def ring_gather(block):
        me = lax.axis_index('tp')
        up = [(i, (i + 1) % tp_size) for i in range(tp_size)]
        down = [(i, (i - 1) % tp_size) for i in range(tp_size)]
        size = block.shape[0]
        whole = jnp.zeros((tp_size * size, block.shape[1]), block.dtype)

        def put(whole, value, owner, at=0):
            return lax.dynamic_update_slice_in_dim(whole, value, (owner % tp_size) * size + at, 0)

        whole = put(whole, block, me)
        left = lax.ppermute(block, 'tp', up)
        right = lax.ppermute(block, 'tp', down)
        far_left = lax.ppermute(left[:size // 2], 'tp', up)
        far_right = lax.ppermute(right[size // 2:], 'tp', down)
        whole = put(whole, left, me + tp_size - 1)
        whole = put(whole, right, me + 1)
        whole = put(whole, far_left, me + 2)
        return put(whole, far_right, me + 2, size // 2)

    def gather_of(ringed):
        return ring_gather if ringed and tp_size == 4 else gather

    def finish(partial, residual, gain, ahead):
        summed = lax.psum_scatter(partial, 'tp', scatter_dimension=0, tiled=True)
        if ahead is not None:
            summed, _ = barrier((summed, ahead))
        return (residual.astype(F32) + rms_norm(summed, gain)).astype(BF16)

    def mlp(u_mlp, w_gate, w_up, w_down):
        gate_pre = jnp.dot(u_mlp, w_gate, preferred_element_type=F32)
        up_pre = jnp.dot(u_mlp, w_up, preferred_element_type=F32)
        hidden_act = (jax.nn.silu(gate_pre) * up_pre).astype(BF16)
        return jnp.dot(hidden_act, w_down, preferred_element_type=F32)

    def after_attention(partial_of, residuals, gain, w_gate, w_up, w_down, send_of, ring_sent):
        mids, gathered, partials, sent = [], [], [], []
        ahead = None
        for c in range(CHUNKS):
            o_partial = partial_of(c)
            if c > 0:
                partials.append(mlp(gathered[-1], w_gate, w_up, w_down))
            x_mid = finish(o_partial, residuals[c], gain[1], ahead)
            mids.append(x_mid)
            ahead = rms_norm(x_mid, gain[2]).astype(BF16)
            gathered.append(gather_of(c == 0)(ahead))
        ahead = None
        for c in range(CHUNKS):
            if c + 1 < CHUNKS:
                follow = gathered[-1]
                follow, partials[c] = barrier((follow, partials[c]))
                gathered[-1] = follow
            else:
                partials.append(mlp(gathered[-1], w_gate, w_up, w_down))
                if not ring_sent:
                    sent[-1], partials[c] = barrier((sent[-1], partials[c]))
            done = finish(partials[c], mids[c], gain[3], ahead)
            mids[c] = done
            ahead = send_of(done)
            sent.append(gather_of(c == 0 and ring_sent)(ahead))
        return mids, sent

    def device_fn(x_loc, pos_loc, gains, w_q, w_k, w_v, w_o, w_gate, w_up, w_down):
        tp_idx = lax.axis_index('tp')
        sp_idx = lax.axis_index('sp')
        tokens, width = x_loc.shape
        rows = tokens // CHUNKS
        part = rows // tp_size
        heads_tp, dim = w_q.shape[2:]
        kv_tp = w_k.shape[2]
        repeat = sp_size // kv_tp
        w_o = barrier(w_o.reshape(w_o.shape[0], heads_tp * dim, width))

        tables = rope_tables(pos_loc, dim // 2, LOCAL_BASE)
        u_norm = rms_norm(x_loc, gains[0, 0]).astype(BF16)
        qkv = project(u_norm, pack_weights(w_q, w_k, w_v, 0), tables, heads_tp + kv_tp)
        kv = qkv[heads_tp:]
        tail = kv[:, tokens - WINDOW:]
        halo = lax.ppermute(tail, 'sp', [(i, i + 1) for i in range(sp_size - 1)])
        first = jnp.where(sp_idx == 0, WINDOW, 0).astype(jnp.int32).reshape(1)
        kv_ext = jnp.concatenate([halo, kv], axis=1)
        residuals = [lax.dynamic_slice_in_dim(x_loc, c * rows + tp_idx * part, part, 0) for c in range(CHUNKS)]
        hidden, u_next = after_attention(
            lambda c: jnp.dot(local_attention(first, qkv, kv_ext, kv_tp, c), w_o[0], preferred_element_type=F32),
            residuals, gains[0], w_gate[0], w_up[0], w_down[0], lambda done: rms_norm(done, gains[1, 0]).astype(BF16), True)

        pairs = tail.reshape(2, kv_tp, WINDOW, dim)
        held = pairs[:, kv_tp - 1]
        for h in range(kv_tp - 1):
            owner = (h + 1) * repeat - 1
            held = jnp.where(sp_idx == owner, lax.ppermute(pairs[:, h], 'sp', [(sp_size - 1, owner)]), held)
        reach = repeat
        while reach > 1:
            moves = [(end - 1, end - 1 - reach // 2) for end in range(reach, sp_size + 1, reach)]
            moved = lax.ppermute(held, 'sp', moves)
            takes = (sp_idx + 1) % reach == reach // 2
            held = jnp.where(takes, moved, held)
            reach //= 2
        k_local = held[0][:, None, :]
        v_local = held[1][:, None, :]

        tables = rope_tables(pos_loc, dim // 2, GLOBAL_BASE)
        packed = pack_weights(w_q, w_k, w_v, 1)
        got = []
        for c in range(CHUNKS):
            qkv = project(u_next[c], packed, tables[:, c * rows:(c + 1) * rows], heads_tp + kv_tp)
            outgoing = jnp.stack([qkv[:heads_tp], jnp.repeat(qkv[heads_tp:heads_tp + kv_tp], repeat, axis=0),
                                  jnp.repeat(qkv[heads_tp + kv_tp:], repeat, axis=0)], axis=1)
            got.append(lax.all_to_all(outgoing, 'sp', 0, 0, tiled=True))
        k_all = jnp.concatenate([g[:, 1] for g in got], axis=1).reshape(sp_size * tokens, dim)
        v_all = jnp.concatenate([g[:, 2] for g in got], axis=1).reshape(sp_size * tokens, dim)

        def global_partial(c):
            back = lax.all_to_all(global_attention(got[c], k_all, v_all, c), 'sp', 0, 0, tiled=True)
            back = back.transpose(1, 0, 2).reshape(rows, heads_tp * dim)
            return jnp.dot(back, w_o[1], preferred_element_type=F32)

        _, outs = after_attention(global_partial, hidden, gains[1], w_gate[1], w_up[1], w_down[1], lambda done: done, False)
        return jnp.concatenate(outs, axis=0), k_local, v_local, k_all[:, None, :], v_all[:, None, :]

    token_spec = P(('rep', 'sp'), None)
    cache_spec = P('rep', ('tp', 'sp'), None)
    in_specs = (token_spec, P(('rep', 'sp')), P(), P(None, None, 'tp', None), P(None, None, 'tp', None),
                P(None, None, 'tp', None), P(None, 'tp', None, None), P(None, None, 'tp'), P(None, None, 'tp'),
                P(None, 'tp', None))
    out_specs = (token_spec, cache_spec, cache_spec, cache_spec, cache_spec)
    return jax.shard_map(device_fn, mesh=mesh, in_specs=in_specs, out_specs=out_specs, check_vma=False)
```
